8 devices in a mesh: hp: 1 (over z), cp: 8 (over y, x, core).
Axes of the slice: x: 2, y: 2, z: 1, core: 2. Of those that a mesh axis runs over, the one named last changes fastest.
Arguments:
- q: bfloat16 [3072, 32, 128], P('cp', 'hp')
- k: bfloat16 [3072, 32, 128], P('cp', 'hp')
- v: bfloat16 [3072, 32, 128], P('cp', 'hp')
- u_bias: float32 [32, 128], P('hp')
- v_bias: float32 [32, 128], P('hp')
- rel_table: bfloat16 [3072, 4096], P('cp')
- w_rel: bfloat16 [4096, 32, 128], P(None, 'hp')
- d_out: bfloat16 [3072, 32, 128], P('cp', 'hp')
Outputs:
- output 1: bfloat16 [3072, 32, 128], P('cp', 'hp')
- output 2: bfloat16 [3072, 32, 128], P('cp', 'hp')
- output 3: bfloat16 [3072, 32, 128], P('cp', 'hp')
- output 4: bfloat16 [3072, 32, 128], P('cp', 'hp')
- output 5: float32 [32, 128], P('hp')
- output 6: float32 [32, 128], P('hp')
- output 7: float32 [4096, 32, 128], P(None, 'hp')
All inputs are finite; a program needn't handle non-finite values.
Results may differ from the reference program's by a relative error of at most 0.016366.
Values are sent between devices in bfloat16 or wider.
A program may use at most 1 GiB of HBM per device.

```python
import math
import jax
import jax.numpy as jnp
from jax import lax

SEQ_LEN = 3072
HEADS_PART = 32
HEAD_DIM = 128
MODEL_DIM = 4096
ROW_BLOCK = math.gcd(SEQ_LEN, 256)
INV_SQRT = HEAD_DIM ** -0.5


def setup_inputs(seed: int = 0, part: int = 0) -> dict:
    part_key = jax.random.fold_in(jax.random.key(seed), part)
    keys_part = jax.random.split(part_key, 7)
    table_keys = jax.random.split(jax.random.key(seed + 17), 2)
    seq_shape = (SEQ_LEN, HEADS_PART, HEAD_DIM)
    head_shape = (HEADS_PART, HEAD_DIM)
    q = jax.random.normal(keys_part[0], seq_shape, jnp.float32)
    k = 2.0 * jax.random.normal(keys_part[1], seq_shape, jnp.float32)
    v = jax.random.normal(keys_part[2], seq_shape, jnp.float32)
    u_bias = 0.5 * jax.random.normal(keys_part[3], head_shape, jnp.float32)
    v_bias = jax.random.normal(keys_part[4], head_shape, jnp.float32)
    w_rel = jax.random.normal(keys_part[5], (MODEL_DIM, HEADS_PART, HEAD_DIM), jnp.float32) * MODEL_DIM ** -0.5
    d_out = jax.random.normal(keys_part[6], seq_shape, jnp.float32)
    freq_cols = 10000.0 ** (-jax.random.uniform(table_keys[0], (MODEL_DIM,), jnp.float32))
    phases = 2.0 * math.pi * jax.random.uniform(table_keys[1], (MODEL_DIM,), jnp.float32)
    offsets = jnp.arange(SEQ_LEN, dtype=jnp.float32)
    rel_table = jnp.sin(offsets[:, None] * freq_cols[None, :] + phases[None, :])
    return {
        'q': q.astype(jnp.bfloat16),
        'k': k.astype(jnp.bfloat16),
        'v': v.astype(jnp.bfloat16),
        'u_bias': u_bias,
        'v_bias': v_bias,
        'rel_table': rel_table.astype(jnp.bfloat16),
        'w_rel': w_rel.astype(jnp.bfloat16),
        'd_out': d_out.astype(jnp.bfloat16),
    }


def attention(q_u, q_v, k, v, rel):
    key_pos = jnp.arange(SEQ_LEN)

    def one_head(head_args):
        qu_h, qv_h, k_h, v_h, rel_h = head_args

        def row_block(start):
            qu_rows = lax.dynamic_slice_in_dim(qu_h, start, ROW_BLOCK)
            qv_rows = lax.dynamic_slice_in_dim(qv_h, start, ROW_BLOCK)
            query_pos = start + jnp.arange(ROW_BLOCK)
            offset_ij = query_pos[:, None] - key_pos[None, :]
            content = jnp.dot(qu_rows, k_h.T)
            by_offset = jnp.dot(qv_rows, rel_h.T)
            position = jnp.take_along_axis(by_offset, jnp.clip(offset_ij, 0, SEQ_LEN - 1), axis=1)
            score_ij = jnp.where(offset_ij >= 0, (content + position) * INV_SQRT, -jnp.inf)
            return jnp.dot(jax.nn.softmax(score_ij, axis=-1), v_h)

        starts = jnp.arange(0, SEQ_LEN, ROW_BLOCK)
        return lax.map(jax.checkpoint(row_block), starts).reshape(SEQ_LEN, HEAD_DIM)

    per_head = lax.map(jax.checkpoint(one_head), tuple(stacked.transpose(1, 0, 2) for stacked in (q_u, q_v, k, v, rel)))
    return per_head.transpose(1, 0, 2)


def reference(q, k, v, u_bias, v_bias, rel_table, w_rel, d_out):
    rel = jnp.dot(rel_table, w_rel.reshape(MODEL_DIM, HEADS_PART * HEAD_DIM), preferred_element_type=jnp.float32)
    rel = rel.astype(jnp.bfloat16).reshape(SEQ_LEN, HEADS_PART, HEAD_DIM)
    q_wide = q.astype(jnp.float32)
    q_u = (q_wide + u_bias).astype(jnp.bfloat16).astype(jnp.float32)
    q_v = (q_wide + v_bias).astype(jnp.bfloat16).astype(jnp.float32)
    out_full, pullback = jax.vjp(attention, q_u, q_v, k.astype(jnp.float32), v.astype(jnp.float32), rel.astype(jnp.float32))
    g_qu, g_qv, g_k, g_v, g_rel = pullback(d_out.astype(jnp.float32))
    d_rel = g_rel.astype(jnp.bfloat16).reshape(SEQ_LEN, HEADS_PART * HEAD_DIM)
    d_w_rel = jnp.dot(rel_table.T, d_rel, preferred_element_type=jnp.float32).reshape(MODEL_DIM, HEADS_PART, HEAD_DIM)
    return (
        out_full.astype(jnp.bfloat16),
        (g_qu + g_qv).astype(jnp.bfloat16),
        g_k.astype(jnp.bfloat16),
        g_v.astype(jnp.bfloat16),
        g_qu.sum(axis=0),
        g_qv.sum(axis=0),
        d_w_rel,
    )
```

```python
import jax
import jax.numpy as jnp
from jax import lax
from jax.experimental import pallas as pl
from jax.experimental.pallas import tpu as pltpu
from jax.sharding import PartitionSpec as P

f32, bf16 = jnp.float32, jnp.bfloat16
VM = pl.BlockSpec(memory_space=pltpu.VMEM)
MIB = 1024 * 1024


def attn_kernel(x_ref, rel_ref, ub_ref, vb_ref, y_ref, drel_ref, du_ref, dv_ref,
                q_s, k_s, v_s, g_s, r_s, kT_s, vT_s, rT_s, dkT_s, dvT_s, drT_s, sc_s, carry_s, acc_s, dcar_s):
    T = q_s.shape[0]
    NB, _, BL, D = x_ref.shape
    Q, C = 256, 512
    nq = T // Q
    scale = D ** -0.5
    c2 = scale * 1.4426950408889634
    for b in range(NB):
        for a, dst in enumerate((q_s, k_s, v_s, g_s)):
            dst[pl.ds(b * BL, BL), :] = x_ref[b, a]
    flip8 = 7 - lax.broadcasted_iota(jnp.int32, (8, 128), 0)

    def flip(x):
        n, w = x.shape
        rows = []
        for g in range(n // 8 - 1, -1, -1):
            rows.append(jnp.concatenate([jnp.take_along_axis(x[8 * g:8 * g + 8, 128 * t:128 * t + 128], flip8, axis=0) for t in range(w // 128)], axis=1))
        return jnp.concatenate(rows, axis=0)

    def flip_rel(c, _):
        o = pl.multiple_of(c * Q, Q)
        r_s[pl.ds(pl.multiple_of(T - Q - c * Q, Q), Q), :] = flip(rel_ref[pl.ds(o, Q), :].astype(f32)).astype(bf16)
        return 0
    lax.fori_loop(0, nq, flip_rel, 0)
    r_s[pl.ds(T, Q), :] = jnp.zeros((Q, D), bf16)
    def tr(c, _):
        o = pl.multiple_of(c * Q, Q)
        for src, dst in ((k_s, kT_s), (v_s, vT_s), (r_s, rT_s)):
            dst[:, pl.ds(o, Q)] = src[pl.ds(o, Q), :].astype(f32).T.astype(bf16)
        for dst in (dkT_s, dvT_s, drT_s):
            dst[:, pl.ds(o, Q)] = jnp.zeros((D, Q), f32)
        return 0
    lax.fori_loop(0, nq, tr, 0)
    rT_s[:, pl.ds(T, Q)] = jnp.zeros((D, Q), bf16)
    drT_s[:, pl.ds(T, Q)] = jnp.zeros((D, Q), f32)
    du_ref[...] = jnp.zeros_like(du_ref)
    dv_ref[...] = jnp.zeros_like(dv_ref)
    def qblock(i, _):
        i0 = pl.multiple_of(i * Q, Q)
        nk = (i + 2) // 2
        w0 = T - Q - i0
        qf = q_s[pl.ds(i0, Q), :].astype(f32)
        quf = (qf + ub_ref[...]).astype(bf16).astype(f32)
        qvf = (qf + vb_ref[...]).astype(bf16).astype(f32)
        qu, qv = quf.astype(bf16), qvf.astype(bf16)
        do = g_s[pl.ds(i0, Q), :]
        dof = do.astype(f32)
        lane = lax.broadcasted_iota(jnp.int32, (Q, Q), 1)
        row = lax.broadcasted_iota(jnp.int32, (Q, Q), 0)
        low = lane < row + 1

        def scores(t, mrun, diag):
            o = pl.multiple_of(t * C, C)
            w = pl.multiple_of(w0 + o, Q)
            b = jnp.dot(qv, rT_s[:, pl.ds(w, C)], preferred_element_type=f32)
            rolled = pltpu.roll(b, C - (Q - 1), 1, stride=1, stride_axis=0)
            right = rolled[:, Q:]
            if diag:
                pos = rolled
            else:
                pos = jnp.concatenate([rolled[:, :Q], jnp.where(low, right, carry_s[...])], axis=1)
            carry_s[...] = right
            s = jnp.dot(qu, kT_s[:, pl.ds(o, C)], preferred_element_type=f32) + pos
            if diag:
                jj = o + lax.broadcasted_iota(jnp.int32, (Q, C), 1)
                ii = i0 + lax.broadcasted_iota(jnp.int32, (Q, C), 0)
                s = jnp.where(jj <= ii, s, -jnp.inf)
            sc_s[:, pl.ds(o, C)] = s
            for u in range(C // 128):
                mrun = jnp.maximum(mrun, s[:, 128 * u:128 * u + 128])
            return mrun
        mrun = scores(nk - 1, jnp.full((Q, 128), -jnp.inf, f32), True)
        mrun = lax.fori_loop(1, nk, lambda tt, m: scores(nk - 1 - tt, m, False), mrun)
        m = jnp.broadcast_to(jnp.max(mrun, axis=1, keepdims=True), (Q, 128))

        def probs(t, st):
            lrun, oacc = st
            o = pl.multiple_of(t * C, C)
            p = []
            for u in range(C // 128):
                pu = jnp.exp2((sc_s[:, pl.ds(o + 128 * u, 128)] - m) * c2)
                lrun = lrun + pu
                sc_s[:, pl.ds(o + 128 * u, 128)] = pu
                p.append(pu.astype(bf16))
            oacc = oacc + jnp.dot(jnp.concatenate(p, axis=1), v_s[pl.ds(o, C), :], preferred_element_type=f32)
            return lrun, oacc
        lrun, oacc = lax.fori_loop(0, nk, probs, (jnp.zeros((Q, 128), f32), jnp.zeros((Q, D), f32)))
        rl = jnp.broadcast_to(1.0 / jnp.sum(lrun, axis=1, keepdims=True), (Q, 128))
        out = oacc * rl
        delta = jnp.broadcast_to(jnp.sum(dof * out, axis=1, keepdims=True), (Q, 128))
        def put(a, val):
            for h in range(Q // 128):
                r0 = i0 + 128 * h
                y_ref[r0 // BL, a, pl.ds(pl.multiple_of(r0 % BL, 128), 128), :] = val[128 * h:128 * h + 128]
        put(0, out.astype(bf16))
        doT, quT = dof.T.astype(bf16), quf.T.astype(bf16)
        qvrT = flip(qvf).T.astype(bf16)
        geq = lane >= row
        dcar_s[...] = jnp.zeros((Q, Q), f32)

        def grads(t, st):
            dqu, dqv = st
            o = pl.multiple_of(t * C, C)
            w = pl.multiple_of(w0 + o, Q)
            dp = jnp.dot(do, vT_s[:, pl.ds(o, C)], preferred_element_type=f32)
            pb, ds = [], []
            for u in range(C // 128):
                pu = sc_s[:, pl.ds(o + 128 * u, 128)] * rl
                pb.append(pu.astype(bf16))
                ds.append(pu * (dp[:, 128 * u:128 * u + 128] - delta))
            pb = jnp.concatenate(pb, axis=1)
            ds = jnp.concatenate(ds, axis=1)
            dsb = ds.astype(bf16)
            dvT_s[:, pl.ds(o, C)] += jnp.dot(doT, pb, preferred_element_type=f32)
            dkT_s[:, pl.ds(o, C)] += jnp.dot(quT, dsb, preferred_element_type=f32)
            dqu = dqu + jnp.dot(dsb, k_s[pl.ds(o, C), :], preferred_element_type=f32)
            rolled = pltpu.roll(flip(ds), 0, 1, stride=1, stride_axis=0)
            left = rolled[:, :Q]
            dw = jnp.concatenate([jnp.where(geq, left, dcar_s[...]), rolled[:, Q:]], axis=1).astype(bf16)
            dcar_s[...] = left
            dqv = dqv + jnp.dot(dw, r_s[pl.ds(w, C), :], preferred_element_type=f32)
            drT_s[:, pl.ds(w, C)] += jnp.dot(qvrT, dw, preferred_element_type=f32)
            return dqu, dqv
        dqu, dqv = lax.fori_loop(0, nk, grads, (jnp.zeros((Q, D), f32), jnp.zeros((Q, D), f32)))
        dqu = dqu * scale
        dqv = flip(dqv) * scale
        put(1, (dqu + dqv).astype(bf16))
        du_ref[...] += jnp.sum(dqu, axis=0, keepdims=True)
        dv_ref[...] += jnp.sum(dqv, axis=0, keepdims=True)
        return 0
    lax.fori_loop(0, nq, qblock, 0)
    for b in range(NB):
        y_ref[b, 2] = (dkT_s[:, pl.ds(b * BL, BL)] * scale).T.astype(bf16)
        y_ref[b, 3] = dvT_s[:, pl.ds(b * BL, BL)].T.astype(bf16)

    def unflip_rel(c, _):
        o = pl.multiple_of(c * Q, Q)
        drel_ref[pl.ds(pl.multiple_of(T - Q - c * Q, Q), Q), :] = flip((drT_s[:, pl.ds(o, Q)] * scale).T).astype(bf16)
        return 0
    lax.fori_loop(0, nq, unflip_rel, 0)

def attn(x, relf, ub, vb):
    NB, _, BL, D = x.shape
    T = NB * BL
    vm = pl.BlockSpec(memory_space=pltpu.VMEM)
    flops = 9 * 2 * T * T // 2 * D
    return pl.pallas_call(
        attn_kernel,
        out_shape=(jax.ShapeDtypeStruct(x.shape, bf16), jax.ShapeDtypeStruct((T, D), bf16),
                   jax.ShapeDtypeStruct((1, D), f32), jax.ShapeDtypeStruct((1, D), f32)),
        in_specs=[vm] * 4, out_specs=(vm,) * 4,
        scratch_shapes=[pltpu.VMEM((T, D), bf16)] * 4 + [pltpu.VMEM((T + 256, D), bf16)]
        + [pltpu.VMEM((D, T), bf16)] * 2 + [pltpu.VMEM((D, T + 256), bf16)]
        + [pltpu.VMEM((D, T), f32)] * 2 + [pltpu.VMEM((D, T + 256), f32)]
        + [pltpu.VMEM((256, T), f32), pltpu.VMEM((256, 256), f32), pltpu.VMEM((256, 256), f32), pltpu.VMEM((256, 256), f32)],
        compiler_params=pltpu.CompilerParams(vmem_limit_bytes=56 * 1024 * 1024),
        cost_estimate=pl.CostEstimate(flops=flops, bytes_accessed=8 * T * D * 2, transcendentals=T * T // 2),
    )(x, relf, ub, vb)


def split_kernel(q_ref, k_ref, v_ref, g_ref, x_ref, buf):
    BL, HB, D = q_ref.shape
    for a, src in enumerate((q_ref, k_ref, v_ref, g_ref)):
        buf[...] = src[...].astype(f32).reshape(BL * HB, D)
        for h in range(HB):
            x_ref[h, a] = buf[pl.ds(h, BL, stride=HB), :].astype(bf16)


def split_heads(q, k, v, g, step, n_dev):
    BL, _, D = q.shape
    return pl.pallas_call(
        split_kernel,
        grid=(1,),
        out_shape=jax.ShapeDtypeStruct((n_dev, 4, BL, D), bf16),
        in_specs=[pl.BlockSpec((BL, n_dev, D), lambda i: (0, step, 0))] * 4,
        out_specs=pl.BlockSpec((n_dev, 4, BL, D), lambda i: (0, 0, 0, 0)),
        scratch_shapes=[pltpu.VMEM((BL * n_dev, D), f32)],
        compiler_params=pltpu.CompilerParams(vmem_limit_bytes=40 * MIB),
        cost_estimate=pl.CostEstimate(flops=10 ** 8, bytes_accessed=16 * n_dev * BL * D, transcendentals=0),
    )(q, k, v, g)


def merge_kernel(*refs):
    z_ref, outs, buf = refs[0], refs[-5:-1], refs[-1]
    HB, _, BL, D = z_ref.shape
    for a, dst in enumerate(outs):
        for h in range(HB):
            buf[pl.ds(h, BL, stride=HB), :] = z_ref[h, a].astype(f32)
        dst[...] = buf[...].reshape(BL, HB, D).astype(bf16)


def merge_heads(z, prev, step, num_heads):
    HB, _, BL, D = z.shape
    out = jax.ShapeDtypeStruct((BL, num_heads, D), bf16)
    ops = (z,) if prev is None else (z, *prev)
    return pl.pallas_call(
        merge_kernel,
        grid=(1,),
        out_shape=(out,) * 4,
        in_specs=[pl.BlockSpec((HB, 4, BL, D), lambda i: (0, 0, 0, 0))] + [pl.BlockSpec(memory_space=pl.ANY)] * (len(ops) - 1),
        out_specs=(pl.BlockSpec((BL, HB, D), lambda i: (0, step, 0)),) * 4,
        scratch_shapes=[pltpu.VMEM((BL * HB, D), f32)],
        input_output_aliases={} if prev is None else {1: 0, 2: 1, 3: 2, 4: 3},
        compiler_params=pltpu.CompilerParams(vmem_limit_bytes=40 * MIB),
        cost_estimate=pl.CostEstimate(flops=10 ** 8, bytes_accessed=16 * HB * BL * D, transcendentals=0),
    )(*ops)


def dw_kernel(t_ref, d_ref, *rest):
    o_ref = rest[-1]
    MB, HB, D = o_ref.shape
    rhs = jnp.concatenate([d_ref[h] for h in range(HB)], axis=1)
    acc = lax.dot_general(t_ref[...], rhs, (((0,), (0,)), ((), ())), preferred_element_type=f32)
    out = o_ref.reshape(MB * HB, D)
    for h in range(HB):
        out[pl.ds(h, MB, stride=HB), :] = acc[:, h * D:(h + 1) * D]


def dw_matmul(table, drel, prev, step, num_heads):
    T, M = table.shape
    HB, _, D = drel.shape
    MB = 256
    ops = (table, drel) if prev is None else (table, drel, prev)
    return pl.pallas_call(
        dw_kernel,
        grid=(M // MB,),
        out_shape=jax.ShapeDtypeStruct((M, num_heads, D), f32),
        in_specs=[pl.BlockSpec((T, MB), lambda i: (0, i)), pl.BlockSpec((HB, T, D), lambda i: (0, 0, 0))] + [pl.BlockSpec(memory_space=pl.ANY)] * (len(ops) - 2),
        out_specs=pl.BlockSpec((MB, HB, D), lambda i: (i, step, 0)),
        input_output_aliases={} if prev is None else {2: 0},
        compiler_params=pltpu.CompilerParams(vmem_limit_bytes=56 * MIB),
        cost_estimate=pl.CostEstimate(flops=2 * T * M * HB * D, bytes_accessed=2 * T * M + 2 * T * HB * D + 4 * M * HB * D, transcendentals=0),
    )(*ops)


def rel_kernel(t_ref, w_ref, o_ref):
    o_ref[...] = jnp.dot(t_ref[...], w_ref[...], preferred_element_type=f32).astype(bf16)


def rel_matmul(table, w):
    T, M = table.shape
    N = w.shape[1]
    TB = 384
    return pl.pallas_call(
        rel_kernel,
        grid=(T // TB,),
        out_shape=jax.ShapeDtypeStruct((T, N), bf16),
        in_specs=[pl.BlockSpec((TB, M), lambda i: (i, 0)), pl.BlockSpec((M, N), lambda i: (0, 0))],
        out_specs=pl.BlockSpec((TB, N), lambda i: (i, 0)),
        compiler_params=pltpu.CompilerParams(vmem_limit_bytes=56 * MIB),
        cost_estimate=pl.CostEstimate(flops=2 * T * M * N, bytes_accessed=2 * (T * M + M * N + T * N), transcendentals=0),
    )(table, w)


def solution(mesh):
    n_dev = mesh.shape['cp']
    seq_spec = P('cp', 'hp', None)
    head_spec = P('hp', None)
    weight_spec = P(None, 'hp', None)

    def local_fn(q, k, v, u_bias, v_bias, rel_table, w_rel, d_out):
        BL, H, D = q.shape
        M = w_rel.shape[0]
        steps = H // n_dev
        me = lax.axis_index('cp')
        table = lax.all_gather(rel_table, 'cp', tiled=True)
        w_own = lax.dynamic_index_in_dim(w_rel.reshape(M, steps, n_dev, D), me, 2, keepdims=False).reshape(M, steps * D)
        ub = lax.dynamic_index_in_dim(u_bias.reshape(steps, n_dev, D), me, 1, keepdims=False)
        vb = lax.dynamic_index_in_dim(v_bias.reshape(steps, n_dev, D), me, 1, keepdims=False)
        xs = [lax.all_to_all(split_heads(q, k, v, d_out, s, n_dev), 'cp', 0, 0) for s in range(steps)]
        rel = rel_matmul(table, w_own)
        outs, dw, sums = None, None, []
        for s in range(steps):
            y, drel, du, dv = attn(xs[s], rel[:, s * D:(s + 1) * D], ub[s:s + 1], vb[s:s + 1])
            sums.append(jnp.stack([du, dv]))
            drel_all = lax.all_gather(drel, 'cp')
            z = lax.all_to_all(y, 'cp', 0, 0)
            dw = dw_matmul(table, drel_all, dw, s, H)
            outs = merge_heads(z, outs, s, H)
        sums = lax.all_gather(jnp.concatenate(sums, axis=1), 'cp')
        sums = sums.transpose(1, 2, 0, 3).reshape(2, H, D)
        return (*outs, sums[0], sums[1], dw)

    return jax.shard_map(
        local_fn,
        mesh=mesh,
        in_specs=(seq_spec, seq_spec, seq_spec, head_spec, head_spec, P('cp', None), weight_spec, seq_spec),
        out_specs=(seq_spec, seq_spec, seq_spec, seq_spec, head_spec, head_spec, weight_spec),
        check_vma=False,
    )
```
